32 devices in a mesh: gx: 4 (over z), gy: 4 (over y, x), gz: 2 (over core).
Axes of the slice: x: 2, y: 2, z: 4, core: 2. Of those that a mesh axis runs over, the one named last changes fastest.
Arguments:
- factor_inv: bfloat16 [4, 4096, 2048], P('gx', 'gy', 'gz')
- sep_sizes: int32 [4, 4, 2], P('gx', 'gy', 'gz'), may hold values from 512 to 1024
- coupling: bfloat16 [12, 4096, 2048], P('gx', 'gy', 'gz'), may hold values from -0.109375 to 0.109375
Outputs:
- schur_update: float32 [4, 4096, 2048], P('gx', 'gy', 'gz')
The draws below stay inside these ranges and needn't reach their ends.
All inputs are finite; a program needn't handle non-finite values.
Results may differ from the reference program's by a relative error of at most 0.0023.
Values may be sent and summed in bfloat16 or wider, within the bound.
A program may use at most 128 MiB of HBM per device.

```python
import jax
import jax.numpy as jnp
from jax import lax

W = 1024
M = 1024
SLOTS = 3
N_GX = 4
N_GY = 4
N_GZ = 2


def draw_factor_inv(key, part):
    first, second = jax.random.split(jax.random.fold_in(key, 11))
    shape = (N_GX, N_GY * W, N_GZ * W)
    rows = lax.broadcasted_iota(jnp.int32, shape, 1) % W
    cols = lax.broadcasted_iota(jnp.int32, shape, 2) % W
    lower = jax.random.normal(first, shape, jnp.float32)
    diag = jax.random.uniform(second, shape, jnp.float32, 0.5, 1.5)
    scaled = lower / jnp.sqrt(jnp.float32(W))
    return jnp.where(rows > cols, scaled, jnp.where(rows == cols, diag, jnp.float32(0.0))).astype(jnp.bfloat16)


def with_ends(entries, key, smallest, high):
    shape = entries.shape
    index_at = [jax.random.randint(jax.random.fold_in(key, axis), (), 0, shape[axis]) for axis in range(len(shape))]
    entries = entries.at[tuple(index_at)].set(smallest)
    longest = shape.index(max(shape))
    index_at[longest] = (index_at[longest] + 1) % shape[longest]
    return entries.at[tuple(index_at)].set(high)


def level_of(own_key, extent, cuts, low, largest):
    def one(dim, blocks):
        steps = jax.random.uniform(jax.random.fold_in(jax.random.fold_in(own_key, 6), dim), (blocks,), jnp.float32, low / len(cuts), largest / len(cuts))
        return jnp.repeat(jnp.exp(steps), extent[dim] // blocks).reshape((-1,) + (1,) * (len(extent) - dim - 1))

    gain = one(*cuts[0])
    for cut in cuts[1:]:
        gain = gain * one(*cut)
    return gain


def gaussian(key, dims, spread, most, cuts=(), held_as=jnp.bfloat16):
    drawn = jax.random.normal(key, dims, jnp.float32) * spread
    if len(cuts) > 0:
        drawn = level_of(key, dims, cuts, -0.22, 0.18) * drawn
    return jnp.clip(drawn, min=-most, max=most).astype(held_as)


def setup_inputs(seed: int = 0) -> dict:
    splits = jax.random.split(jax.random.key(seed), 4)
    factor_inv = draw_factor_inv(jax.random.fold_in(splits[3], 71), 0)
    sep_sizes = with_ends(jax.random.randint(splits[1], (N_GX, N_GY, N_GZ), W // 2, W + 1), jax.random.fold_in(splits[1], 1), W // 2, W).astype(jnp.int32)
    coupling = gaussian(splits[2], (N_GX * SLOTS, N_GY * W, N_GZ * M), (3 * W) ** -0.5, 0.109375, ((0, 4), (1, 4), (2, 2)))
    return dict(factor_inv=factor_inv, sep_sizes=sep_sizes, coupling=coupling)


def reference(factor_inv, sep_sizes, coupling):
    nxa = factor_inv.shape[0]
    nya = factor_inv.shape[1] // W
    nza = factor_inv.shape[2] // W
    inner = jnp.arange(W, dtype=jnp.int32)

    def owned(iidx, jidx, kidx):
        valid = (jidx >= 0) & (jidx < nya) & (kidx >= 0) & (kidx < nza)
        jc = jnp.clip(jidx, 0, nya - 1).astype(jnp.int32)
        kc = jnp.clip(kidx, 0, nza - 1).astype(jnp.int32)
        block = lax.dynamic_slice(factor_inv, (iidx, jc * W, kc * W), (1, W, W))[0]
        count = lax.dynamic_slice(sep_sizes, (iidx, jc, kc), (1, 1, 1))[0, 0, 0]
        keep = ((inner < count) & valid).astype(jnp.bfloat16)
        return block * keep[:, None] * keep[None, :]

    def one(flat):
        iidx = (flat // (nya * nza)).astype(jnp.int32)
        jidx = ((flat // nza) % nya).astype(jnp.int32)
        kidx = (flat % nza).astype(jnp.int32)
        cblock = lax.dynamic_slice(coupling, (iidx * 3, jidx * W, kidx * M), (3, W, M))
        factors = [owned(iidx, jidx, kidx - 1), owned(iidx, jidx, kidx + 1), owned(iidx, jidx - 1, kidx)]
        total = jnp.zeros((M, M), jnp.float32)
        for slot in range(3):
            solved = jnp.dot(factors[slot], cblock[slot], preferred_element_type=jnp.float32).astype(jnp.bfloat16)
            total = total + jnp.dot(solved.T, solved, preferred_element_type=jnp.float32)
        return total

    result = lax.map(one, jnp.arange(nxa * nya * nza, dtype=jnp.int32))
    result = result.reshape(nxa, nya, nza, M, M).transpose(0, 1, 3, 2, 4)
    return result.reshape(nxa, nya * M, nza * M)
```

```python
import functools

import jax
import jax.numpy as jnp
from jax import lax
from jax.experimental import pallas as pl
from jax.experimental.pallas import tpu as pltpu
from jax.sharding import PartitionSpec as P

MESH = pl.DeviceIdType.MESH
F32, BF16 = jnp.float32, jnp.bfloat16
DIAG = 16
TAIL = 128


def dot(lhs, rhs, left, right):
    return lax.dot_general(lhs, rhs, (((left,), (right,)), ((), ())), preferred_element_type=F32)


def split(value):
    high = value.astype(BF16)
    return high, (value - high.astype(F32)).astype(BF16)


def gather_kernel(
    ny, nz, pieces,
    sizes, factor, coupling,
    part_out, tail_out,
    own, couple, beside, solved, total, packed, cross, packed_in, cross_in, full, lows,
    load_sem, z_send, z_recv, y_send, y_recv, store_sem,
):
    width = own.shape[0]
    half = width // 2
    block = half // 2
    steps = width // block
    b, c = lax.axis_index("gy"), lax.axis_index("gz")
    above, below = b < ny - 1, b > 0
    ups, downs = c < nz - 1, c > 0
    peers = ((above, {"gy": b + 1}), (below, {"gy": b - 1}), (ups, {"gz": c + 1}), (downs, {"gz": c - 1}))

    load_factor = pltpu.make_async_copy(factor.at[0], own, load_sem.at[3])
    load_factor.start()
    loads = [pltpu.make_async_copy(coupling.at[e], couple.at[e], load_sem.at[e]) for e in range(3)]
    for load in loads:
        load.start()

    barrier = pltpu.get_barrier_semaphore()
    for there, peer in peers:
        @pl.when(there)
        def _():
            pl.semaphore_signal(barrier, inc=1, device_id=peer, device_id_type=MESH)

    load_factor.wait()
    size = sizes[0, 0, 0]
    column = lax.broadcasted_iota(jnp.int32, (1, width), 1) < size
    diag = jnp.zeros((1, width), F32)
    for s in range(steps):
        rows = pl.ds(s * block, block)
        row = lax.broadcasted_iota(jnp.int32, (block, 1), 0) + s * block < size
        kept = own[rows, :].astype(F32) * row.astype(F32) * column.astype(F32)
        own[rows, :] = kept.astype(BF16)
        diag = diag + jnp.sum(kept * kept, axis=0, keepdims=True)

    pl.semaphore_wait(barrier, sum(there.astype(jnp.int32) for there, _ in peers))

    z_copies = []
    for k, (goes, to, comes) in enumerate(((ups, c + 1, downs), (downs, c - 1, ups))):
        copy = pltpu.make_async_remote_copy(
            src_ref=own, dst_ref=beside.at[k if nz > 2 else 0], send_sem=z_send.at[k], recv_sem=z_recv.at[k],
            device_id={"gz": to}, device_id_type=MESH,
        )
        z_copies.append((goes, comes, copy))

        @pl.when(goes)
        def _():
            copy.start()

    def y_copy(src, dst, k):
        return pltpu.make_async_remote_copy(
            src_ref=src, dst_ref=dst, send_sem=y_send.at[k], recv_sem=y_recv.at[k],
            device_id={"gy": b + 1}, device_id_type=MESH,
        )

    y_copies = [y_copy(packed, packed_in, 0)]
    for k, (start, count) in enumerate(pieces):
        rows = pl.ds(start, count)
        dst = cross_in.at[rows] if k < len(pieces) - 1 else tail_out
        y_copies.append(y_copy(cross.at[rows], dst, k + 1))

    @pl.when(above)
    def _():
        line = lax.broadcasted_iota(jnp.int32, (DIAG, half), 0)
        high = diag.astype(BF16).astype(F32)
        low = diag - high
        rows = (high[:, :half], high[:, half:], low[:, :half], low[:, half:])
        lines = jnp.zeros((DIAG, half), F32)
        for i, value in enumerate(rows):
            lines = jnp.where(line == i, value, lines)
        packed[pl.ds(half, DIAG), :] = lines.astype(BF16)
        for s in range(2):
            rows = lax.broadcasted_iota(jnp.int32, (block, half), 0) + s * block
            cols = lax.broadcasted_iota(jnp.int32, (block, half), 1)
            first = dot(own[:, pl.ds(s * block, block)], own[:, :half], 0, 0)
            second = dot(own[:, pl.ds(half + s * block, block)], own[:, half:], 0, 0)
            mixed = jnp.where(rows < cols, first, jnp.where(rows > cols, second, 0.0))
            packed[pl.ds(s * block, block), :] = mixed.astype(BF16)
        y_copies[0].start()
        for k, (start, count) in enumerate(pieces):
            cross[pl.ds(start, count), :] = dot(own[:, pl.ds(start, count)], own[:, half:], 0, 0).astype(BF16)
            y_copies[k + 1].start()

    for load in loads:
        load.wait()

    def z_slot(slot, k, fresh):
        @pl.loop(0, steps)
        def _(s):
            at = pl.ds(pl.multiple_of(s * block, block), block)
            solved[at, :] = dot(couple[slot, :, at], beside[k], 0, 1).astype(BF16)

        @pl.loop(0, steps)
        def _(s):
            at = pl.ds(pl.multiple_of(s * block, block), block)
            term = dot(solved[at, :], solved[...], 1, 1)
            total[at, :] = term if fresh else total[at, :] + term

    if nz == 2:
        for goes, comes, copy in z_copies:
            @pl.when(comes)
            def _():
                copy.wait_recv()
        z_slot(1 - c, 0, True)
    else:
        total[...] = jnp.zeros_like(total)
        for k, (goes, comes, copy) in enumerate(z_copies):
            @pl.when(comes)
            def _():
                copy.wait_recv()
                z_slot(k, k, False)

    stores = [
        pltpu.make_async_copy(
            total.at[pl.ds(s * block, block)], part_out.at[pl.ds(s * block, block)], store_sem.at[s]
        )
        for s in range(steps)
    ]

    @pl.when(below)
    def _():
        y_copies[0].wait_recv()
        rows = lax.broadcasted_iota(jnp.int32, (half, half), 0)
        cols = lax.broadcasted_iota(jnp.int32, (half, half), 1)
        mixed = packed_in[:half, :].astype(F32)
        lines = packed_in[pl.ds(half, DIAG), :].astype(F32)
        for i, keep in enumerate((rows < cols, rows > cols)):
            one = jnp.where(keep, mixed, 0.0)
            both = one + one.T + jnp.where(rows == cols, lines[i : i + 1, :], 0.0)
            full[i] = both.astype(BF16)
            lows[i] = jnp.where(rows == cols, lines[i + 2 : i + 3, :], 0.0).astype(BF16)

        @pl.loop(0, steps)
        def _(s):
            at = pl.ds(pl.multiple_of(s * block, block), block)
            term = total[at, :]
            for i in range(2):
                piece = couple[2, pl.ds(i * half, half), at]
                high, low = split(dot(piece, full[i], 0, 0) + dot(piece, lows[i], 0, 0))
                rest = couple[2, pl.ds(i * half, half), :]
                term = term + dot(high, rest, 1, 0) + dot(low, rest, 1, 0)
            total[at, :] = term

        for k, (start, count) in enumerate(pieces[:-1]):
            y_copies[k + 1].wait_recv()
            rows = pl.ds(start, count)
            high, low = split(dot(cross_in[rows, :], couple[2, pl.ds(half, half), :], 1, 0))
            mine = couple[2, rows, :]
            for i, value in enumerate((mine, mine, high, low)):
                solved[pl.ds(i * count, count), :] = value
            last = k == len(pieces) - 2
            for s in range(steps):
                at = pl.ds(s * block, block)
                term = dot(solved[pl.ds(0, 2 * count), at], solved[pl.ds(2 * count, 2 * count), :], 0, 0)
                term = term + dot(solved[pl.ds(2 * count, 2 * count), at], solved[pl.ds(0, 2 * count), :], 0, 0)
                total[at, :] = total[at, :] + term
                if last:
                    stores[s].start()

    @pl.when(jnp.logical_not(below))
    def _():
        for store in stores:
            store.start()

    @pl.when(below)
    def _():
        y_copies[-1].wait_recv()

    for goes, comes, copy in z_copies:
        @pl.when(goes)
        def _():
            copy.wait_send()

    @pl.when(above)
    def _():
        for copy in y_copies:
            copy.wait_send()

    for store in stores:
        store.wait()


def finish_kernel(tail, mine, rest, part, out, left, right):
    count = tail.shape[0]

    @pl.when(pl.program_id(0) == 0)
    def _():
        held = jnp.where(lax.axis_index("gy") > 0, tail[...].astype(F32), 0.0).astype(BF16)
        high, low = split(dot(held, rest[0], 1, 0))
        for i, (one, other) in enumerate(((mine[0], high), (mine[0], low), (high, mine[0]), (low, mine[0]))):
            left[pl.ds(i * count, count), :] = one
            right[pl.ds(i * count, count), :] = other

    block = out.shape[1]
    at = pl.ds(pl.multiple_of(pl.program_id(0) * block, block), block)
    out[0] = part[...] + dot(left[:, at], right[...], 0, 0)


def on_device(factor_inv, sep_sizes, coupling):
    ny, nz = lax.axis_size("gy"), lax.axis_size("gz")
    width = factor_inv.shape[1]
    inter = coupling.shape[2]
    half = width // 2
    block = half // 2
    steps = width // block
    tail = min(TAIL, block)
    pieces = [(0, block)] + [(start, tail) for start in range(block, half, tail)]
    count = len(pieces) + 1
    anywhere = pl.BlockSpec(memory_space=pl.ANY)
    part, last = pl.pallas_call(
        functools.partial(gather_kernel, ny, nz, pieces),
        out_shape=(
            jax.ShapeDtypeStruct((inter, inter), F32),
            jax.ShapeDtypeStruct((tail, half), BF16),
        ),
        in_specs=[pl.BlockSpec(memory_space=pltpu.SMEM), anywhere, anywhere],
        out_specs=(anywhere, anywhere),
        scratch_shapes=[
            pltpu.VMEM((width, width), BF16),
            pltpu.VMEM((3, width, inter), BF16),
            pltpu.VMEM((2 if nz > 2 else 1, width, width), BF16),
            pltpu.VMEM((inter, width), BF16),
            pltpu.VMEM((inter, inter), F32),
            pltpu.VMEM((half + DIAG, half), BF16),
            pltpu.VMEM((half, half), BF16),
            pltpu.VMEM((half + DIAG, half), BF16),
            pltpu.VMEM((half, half), BF16),
            pltpu.VMEM((2, half, half), BF16),
            pltpu.VMEM((2, half, half), BF16),
            pltpu.SemaphoreType.DMA((4,)),
            pltpu.SemaphoreType.DMA((2,)),
            pltpu.SemaphoreType.DMA((2,)),
            pltpu.SemaphoreType.DMA((count,)),
            pltpu.SemaphoreType.DMA((count,)),
            pltpu.SemaphoreType.DMA((steps,)),
        ],
        compiler_params=pltpu.CompilerParams(
            collective_id=0, has_side_effects=True, vmem_limit_bytes=56 * 2**20
        ),
    )(sep_sizes, factor_inv, coupling)
    rows = block
    return pl.pallas_call(
        finish_kernel,
        grid=(inter // rows,),
        out_shape=jax.ShapeDtypeStruct((1, inter, inter), F32),
        in_specs=[
            pl.BlockSpec((tail, half), lambda s: (0, 0)),
            pl.BlockSpec((1, tail, inter), lambda s: (2, half // tail - 1, 0)),
            pl.BlockSpec((1, half, inter), lambda s: (2, 1, 0)),
            pl.BlockSpec((rows, inter), lambda s: (s, 0)),
        ],
        out_specs=pl.BlockSpec((1, rows, inter), lambda s: (0, s, 0)),
        scratch_shapes=[pltpu.VMEM((4 * tail, inter), BF16), pltpu.VMEM((4 * tail, inter), BF16)],
        compiler_params=pltpu.CompilerParams(vmem_limit_bytes=56 * 2**20),
    )(last, coupling, coupling, part)


def solution(mesh):
    return jax.shard_map(
        on_device,
        mesh=mesh,
        in_specs=(P("gx", "gy", "gz"), P("gx", "gy", "gz"), P("gx", "gy", "gz")),
        out_specs=P("gx", "gy", "gz"),
        check_vma=False,
    )
```

```python
import functools

import jax
import jax.numpy as jnp
from jax import lax
from jax.experimental import pallas as pl
from jax.experimental.pallas import tpu as pltpu
from jax.sharding import PartitionSpec as P

MESH = pl.DeviceIdType.MESH
F32, BF16 = jnp.float32, jnp.bfloat16
DIAG = 16
TAIL = 128


def dot(lhs, rhs, left, right):
    return lax.dot_general(lhs, rhs, (((left,), (right,)), ((), ())), preferred_element_type=F32)


def gather_kernel(
    ny, nz, pieces,
    sizes, factor, coupling,
    part_out, tail_out,
    own, couple, beside, solved, total, packed, cross, packed_in, cross_in, full, lows,
    load_sem, z_send, z_recv, y_send, y_recv, store_sem,
):
    width = own.shape[0]
    half = width // 2
    block = half // 2
    steps = width // block
    b, c = lax.axis_index("gy"), lax.axis_index("gz")
    above, below = b < ny - 1, b > 0
    ups, downs = c < nz - 1, c > 0
    peers = ((above, {"gy": b + 1}), (below, {"gy": b - 1}), (ups, {"gz": c + 1}), (downs, {"gz": c - 1}))

    rows_of = [pl.ds(s * block, block) for s in range(steps)]
    factors = [pltpu.make_async_copy(factor.at[0, at], own.at[at], load_sem.at[3 + s]) for s, at in enumerate(rows_of)]
    for load in factors:
        load.start()
    loads = [pltpu.make_async_copy(coupling.at[e], couple.at[e], load_sem.at[e]) for e in range(3)]

    barrier = pltpu.get_barrier_semaphore()
    for there, peer in peers:
        @pl.when(there)
        def _():
            pl.semaphore_signal(barrier, inc=1, device_id=peer, device_id_type=MESH)

    size = sizes[0, 0, 0]
    column = lax.broadcasted_iota(jnp.int32, (1, width), 1) < size
    diag = jnp.zeros((1, width), F32)
    for s in range(steps):
        rows = rows_of[s]
        factors[s].wait()
        row = lax.broadcasted_iota(jnp.int32, (block, 1), 0) + s * block < size
        kept = own[rows, :].astype(F32) * row.astype(F32) * column.astype(F32)
        own[rows, :] = kept.astype(BF16)
        diag = diag + jnp.sum(kept * kept, axis=0, keepdims=True)

    for load in loads:
        load.start()
    pl.semaphore_wait(barrier, sum(there.astype(jnp.int32) for there, _ in peers))

    z_copies = []
    for k, (goes, to, comes) in enumerate(((ups, c + 1, downs), (downs, c - 1, ups))):
        copy = pltpu.make_async_remote_copy(
            src_ref=own, dst_ref=beside.at[k if nz > 2 else 0], send_sem=z_send.at[k], recv_sem=z_recv.at[k],
            device_id={"gz": to}, device_id_type=MESH,
        )
        z_copies.append((goes, comes, copy))

        @pl.when(goes)
        def _():
            copy.start()

    def y_copy(src, dst, k):
        return pltpu.make_async_remote_copy(
            src_ref=src, dst_ref=dst, send_sem=y_send.at[k], recv_sem=y_recv.at[k],
            device_id={"gy": b + 1}, device_id_type=MESH,
        )

    y_copies = [y_copy(packed, packed_in, 0)]
    for k, (start, count) in enumerate(pieces):
        rows = pl.ds(start, count)
        dst = cross_in.at[rows] if k < len(pieces) - 1 else tail_out
        y_copies.append(y_copy(cross.at[rows], dst, k + 1))

    @pl.when(above)
    def _():
        def send_cross(k):
            start, count = pieces[k]
            cross[pl.ds(start, count), :] = dot(own[:, pl.ds(start, count)], own[:, half:], 0, 0).astype(BF16)
            y_copies[k + 1].start()

        send_cross(0)
        line = lax.broadcasted_iota(jnp.int32, (DIAG, half), 0)
        high = diag.astype(BF16).astype(F32)
        low = diag - high
        rows = (high[:, :half], high[:, half:], low[:, :half], low[:, half:])
        lines = jnp.zeros((DIAG, half), F32)
        for i, value in enumerate(rows):
            lines = jnp.where(line == i, value, lines)
        packed[pl.ds(half, DIAG), :] = lines.astype(BF16)
        for s in range(2):
            rows = lax.broadcasted_iota(jnp.int32, (block, half), 0) + s * block
            cols = lax.broadcasted_iota(jnp.int32, (block, half), 1)
            first = dot(own[:, pl.ds(s * block, block)], own[:, :half], 0, 0)
            second = dot(own[:, pl.ds(half + s * block, block)], own[:, half:], 0, 0)
            mixed = jnp.where(rows < cols, first, jnp.where(rows > cols, second, 0.0))
            packed[pl.ds(s * block, block), :] = mixed.astype(BF16)
        y_copies[0].start()
        for k in range(1, len(pieces)):
            send_cross(k)

    for load in loads:
        load.wait()

    def z_slot(slot, k, fresh):
        @pl.loop(0, steps)
        def _(s):
            at = pl.ds(pl.multiple_of(s * block, block), block)
            solved[at, :] = dot(couple[slot, :, at], beside[k], 0, 1).astype(BF16)

        @pl.loop(0, steps)
        def _(s):
            at = pl.ds(pl.multiple_of(s * block, block), block)
            term = dot(solved[at, :], solved[...], 1, 1)
            total[at, :] = term if fresh else total[at, :] + term

    if nz == 2:
        for goes, comes, copy in z_copies:
            @pl.when(comes)
            def _():
                copy.wait_recv()
        z_slot(1 - c, 0, True)
    else:
        total[...] = jnp.zeros_like(total)
        for k, (goes, comes, copy) in enumerate(z_copies):
            @pl.when(comes)
            def _():
                copy.wait_recv()
                z_slot(k, k, False)

    stores = [
        pltpu.make_async_copy(
            total.at[pl.ds(s * block, block)], part_out.at[pl.ds(s * block, block)], store_sem.at[s]
        )
        for s in range(steps)
    ]

    @pl.when(below)
    def _():
        y_copies[0].wait_recv()
        rows = lax.broadcasted_iota(jnp.int32, (half, half), 0)
        cols = lax.broadcasted_iota(jnp.int32, (half, half), 1)
        mixed = packed_in[:half, :].astype(F32)
        lines = packed_in[pl.ds(half, DIAG), :].astype(F32)
        for i, keep in enumerate((rows < cols, rows > cols)):
            one = jnp.where(keep, mixed, 0.0)
            both = one + one.T + jnp.where(rows == cols, lines[i : i + 1, :], 0.0)
            full[i] = both.astype(BF16)
            lows[i] = jnp.where(rows == cols, lines[i + 2 : i + 3, :], 0.0).astype(BF16)

        @pl.loop(0, steps)
        def _(s):
            at = pl.ds(pl.multiple_of(s * block, block), block)
            term = total[at, :]
            for i in range(2):
                piece = couple[2, pl.ds(i * half, half), at]
                high = (dot(piece, full[i], 0, 0) + dot(piece, lows[i], 0, 0)).astype(BF16)
                rest = couple[2, pl.ds(i * half, half), :]
                term = term + dot(high, rest, 1, 0)
            total[at, :] = term

        for k, (start, count) in enumerate(pieces[:-1]):
            y_copies[k + 1].wait_recv()
            rows = pl.ds(start, count)
            high = dot(cross_in[rows, :], couple[2, pl.ds(half, half), :], 1, 0).astype(BF16)
            mine = couple[2, rows, :]
            for i, value in enumerate((mine, high, mine)):
                solved[pl.ds(i * count, count), :] = value
            last = k == len(pieces) - 2
            for s in range(steps):
                at = pl.ds(s * block, block)
                term = dot(solved[pl.ds(0, 2 * count), at], solved[pl.ds(count, 2 * count), :], 0, 0)
                total[at, :] = total[at, :] + term
                if last:
                    stores[s].start()

    @pl.when(jnp.logical_not(below))
    def _():
        for store in stores:
            store.start()

    @pl.when(below)
    def _():
        y_copies[-1].wait_recv()

    for goes, comes, copy in z_copies:
        @pl.when(goes)
        def _():
            copy.wait_send()

    @pl.when(above)
    def _():
        for copy in y_copies:
            copy.wait_send()

    for store in stores:
        store.wait()


def finish_kernel(tail, mine, rest, part, out, left, right):
    count = tail.shape[0]

    @pl.when(pl.program_id(0) == 0)
    def _():
        held = jnp.where(lax.axis_index("gy") > 0, tail[...].astype(F32), 0.0).astype(BF16)
        high = dot(held, rest[0], 1, 0).astype(BF16)
        for i, (one, other) in enumerate(((mine[0], high), (high, mine[0]))):
            left[pl.ds(i * count, count), :] = one
            right[pl.ds(i * count, count), :] = other

    block = out.shape[1]
    at = pl.ds(pl.multiple_of(pl.program_id(0) * block, block), block)
    out[0] = part[...] + dot(left[:, at], right[...], 0, 0)


def on_device(factor_inv, sep_sizes, coupling):
    ny, nz = lax.axis_size("gy"), lax.axis_size("gz")
    width = factor_inv.shape[1]
    inter = coupling.shape[2]
    half = width // 2
    block = half // 2
    steps = width // block
    tail = min(TAIL, block)
    pieces = [(start, tail) for start in range(0, half, tail)]
    count = len(pieces) + 1
    anywhere = pl.BlockSpec(memory_space=pl.ANY)
    part, last = pl.pallas_call(
        functools.partial(gather_kernel, ny, nz, pieces),
        out_shape=(
            jax.ShapeDtypeStruct((inter, inter), F32),
            jax.ShapeDtypeStruct((tail, half), BF16),
        ),
        in_specs=[pl.BlockSpec(memory_space=pltpu.SMEM), anywhere, anywhere],
        out_specs=(anywhere, anywhere),
        scratch_shapes=[
            pltpu.VMEM((width, width), BF16),
            pltpu.VMEM((3, width, inter), BF16),
            pltpu.VMEM((2 if nz > 2 else 1, width, width), BF16),
            pltpu.VMEM((inter, width), BF16),
            pltpu.VMEM((inter, inter), F32),
            pltpu.VMEM((half + DIAG, half), BF16),
            pltpu.VMEM((half, half), BF16),
            pltpu.VMEM((half + DIAG, half), BF16),
            pltpu.VMEM((half, half), BF16),
            pltpu.VMEM((2, half, half), BF16),
            pltpu.VMEM((2, half, half), BF16),
            pltpu.SemaphoreType.DMA((3 + steps,)),
            pltpu.SemaphoreType.DMA((2,)),
            pltpu.SemaphoreType.DMA((2,)),
            pltpu.SemaphoreType.DMA((count,)),
            pltpu.SemaphoreType.DMA((count,)),
            pltpu.SemaphoreType.DMA((steps,)),
        ],
        compiler_params=pltpu.CompilerParams(
            collective_id=0, has_side_effects=True, vmem_limit_bytes=56 * 2**20
        ),
    )(sep_sizes, factor_inv, coupling)
    rows = block
    return pl.pallas_call(
        finish_kernel,
        grid=(inter // rows,),
        out_shape=jax.ShapeDtypeStruct((1, inter, inter), F32),
        in_specs=[
            pl.BlockSpec((tail, half), lambda s: (0, 0)),
            pl.BlockSpec((1, tail, inter), lambda s: (2, half // tail - 1, 0)),
            pl.BlockSpec((1, half, inter), lambda s: (2, 1, 0)),
            pl.BlockSpec((rows, inter), lambda s: (s, 0)),
        ],
        out_specs=pl.BlockSpec((1, rows, inter), lambda s: (0, s, 0)),
        scratch_shapes=[pltpu.VMEM((2 * tail, inter), BF16), pltpu.VMEM((2 * tail, inter), BF16)],
        compiler_params=pltpu.CompilerParams(vmem_limit_bytes=56 * 2**20),
    )(last, coupling, coupling, part)


def solution(mesh):
    return jax.shard_map(
        on_device,
        mesh=mesh,
        in_specs=(P("gx", "gy", "gz"), P("gx", "gy", "gz"), P("gx", "gy", "gz")),
        out_specs=P("gx", "gy", "gz"),
        check_vma=False,
    )
```
